32 devices in a mesh: rep: 4 (over x, core), fsdp: 2 (over y), exp: 4 (over z).
Axes of the slice: x: 2, y: 2, z: 4, core: 2. Of those that a mesh axis runs over, the one named last changes fastest.
Arguments:
- tok_grad: bfloat16 [4096, 1440], P(('rep', 'fsdp', 'exp')), may hold values from -18 to 18
- expert_ids: int32 [4096, 4], P(('rep', 'fsdp', 'exp')), may hold values from 0 to 127, all different within a row; in each aligned block of 128 rows (0 to 127, 128 to 255, ...) at most 6 rows name the same one
- route_probs: bfloat16 [4096, 4], P(('rep', 'fsdp', 'exp')), may hold values from 0.049804688 to 1
- hidden_slots: bfloat16 [8, 4, 24, 1440], P(('rep', 'fsdp'), 'exp'), may hold values from -17 to 17
- down_weight: bfloat16 [4, 1440, 1440], P('exp', 'fsdp'), may hold values from -0.15625 to 0.15625
Outputs:
- route_grad: float32 [4096, 4], P(('rep', 'fsdp', 'exp'))
- hidden_grad: bfloat16 [8, 4, 24, 1440], P(('rep', 'fsdp'), 'exp')
- weight_grad: bfloat16 [4, 4, 1440, 1440], P('rep', 'exp', 'fsdp')
The draws below stay inside these ranges and needn't reach their ends.
Inputs may be any that keep to these rules, and one draw needn't show every extreme that they name: `expert_ids`: each row names 4 different experts. Of one device's rows at most 6 pairs name any one expert, and in every draw some device's rows reach 6 for some expert. Only experts below 4 are handled here.
All inputs are finite; a program needn't handle non-finite values. Where the reference program divides by a largest or mean magnitude, that divisor is 1e-20 or more.
Results may differ from the reference program's by a relative error of at most 0.005.
Values may be sent and summed in bfloat16 or wider, within the bound.
No kernel may reach another device: no remote copies, remote signals or barrier semaphores. Data moves between devices by JAX's collectives and lax.ppermute only.
A program may use at most 64 MiB of HBM per device.

```python
import math
import jax
import jax.numpy as jnp
import numpy as np
from jax import lax

D = 1440
H = 1440
EXP_ALL = 128
TOP = 4
TOK_DEV = 128
CAP = 6
EXPERTS = 4
SLOTS = 24
GROUPS = 8
TOKENS = 4096
N_REP = 4
N_FSDP = 2
N_EXP = 4


def draw_tok_grad(key, part):
    first_key = jax.random.fold_in(key, 0)
    group_index = jnp.arange(TOKENS) // (TOK_DEV * EXPERTS)
    level = 3.0 ** (group_index.astype(jnp.float32) / max(GROUPS - 1, 1))
    values = jnp.clip(jax.random.normal(first_key, (TOKENS, D), jnp.float32), -6.0, 6.0)
    return (values * level[:, None]).astype(jnp.bfloat16)


def draw_hidden_slots(key, part):
    base_key, level_key = jax.random.split(jax.random.fold_in(key, 7))
    spread = jax.random.uniform(level_key, (EXPERTS,), jnp.float32, -3.0, 1.0)
    levels = jnp.exp(spread)
    full_shape = (GROUPS, EXPERTS, SLOTS, H)
    values = jnp.clip(jax.random.normal(base_key, full_shape, jnp.float32), -6.0, 6.0)
    return (values * levels[None, :, None, None]).astype(jnp.bfloat16)


def shard_levels(own_key, dims, pieces, smallest, largest):
    level, own = 1.0, jax.random.fold_in(own_key, 6)
    for position, shards_of in pieces:
        steps = jnp.exp(jax.random.uniform(jax.random.fold_in(own, position), (shards_of,), jnp.float32, smallest / len(pieces), largest / len(pieces)))
        level = level * jnp.repeat(steps, dims[position] // shards_of).reshape([-1 if axis == position else 1 for axis in range(len(dims))])
    return level


def routed_block(stream_key, own, number, rows, count, top, bound, lean):
    order = jax.random.permutation(stream_key, count)
    packed, usual = load_shares(count, rows * top, bound, lean, True), load_shares(count, rows * top, bound, lean, False)
    places = jnp.arange(count)

    def named(sizes, rotation):
        used = int((sizes > 0).sum())
        fixed = max(1, used // 4)
        moved = fixed + (places - fixed + rotation * (used - fixed)) % max(1, count - fixed)
        return jnp.zeros((count,), jnp.int32).at[order[jnp.where(places < fixed, places, moved)]].set(jnp.asarray(sizes, jnp.int32))

    sizes = jnp.where(number % 4 == 0, named(packed, number // 4), named(usual, number - number // 4 - 1))
    mixed = jax.random.permutation(jax.random.fold_in(own, 3), count)
    source_of, taker = mixed[0:count // 2 * 2:2], mixed[1:count // 2 * 2:2]
    slack = jnp.minimum(sizes[source_of] - 1, bound - sizes[taker]) // 2
    slack = jnp.where((source_of == order[0]) | (taker == order[0]) | (sizes[taker] == 0), 0, jnp.maximum(slack, 0))
    moved = jax.random.randint(jax.random.fold_in(own, 4), (count // 2,), 0, 1 << 20) % (slack + 1)
    sizes = sizes.at[source_of].add(-moved).at[taker].add(moved)
    members = jnp.searchsorted(jnp.cumsum(sizes), jnp.arange(rows * top), side="right").astype(jnp.int32)
    listing = members.reshape(top, rows).T
    listing = listing[jax.random.permutation(jax.random.fold_in(own, 1), rows)]
    rotation = jax.random.randint(jax.random.fold_in(own, 2), (rows, 1), 0, top)
    return jnp.take_along_axis(listing, (jnp.arange(top)[None, :] + rotation) % top, axis=1)


def load_shares(number_of, total, reach, lean, full):
    portions = [(1 << 20) // math.isqrt(standing ** lean) + 1 for standing in range(1, number_of + 1)]
    largest = reach if full else min(reach, max(-(-total // number_of), total * portions[0] // sum(portions)))
    least = 1 if total - largest >= number_of - 1 else 0
    counts, surplus = [largest] + [least] * (number_of - 1), total - largest - least * (number_of - 1)
    while surplus > 0:
        free = [i for i in range(1, number_of) if counts[i] < largest] or [i for i in range(1, number_of) if counts[i] < reach]
        pool, budget = sum([portions[i] for i in free]), surplus
        for i in free:
            more = min(reach - counts[i], max(1, budget * portions[i] // pool), surplus)
            counts[i] = counts[i] + more
            surplus = surplus - more
    return np.array(counts)


def noise(rng, shape, deviation, reach, pieces=(), kind=jnp.bfloat16):
    values = jax.random.normal(rng, shape, jnp.float32) * deviation
    if len(pieces) > 0:
        values = shard_levels(rng, shape, pieces, -0.22, 0.18) * values
    return jnp.clip(values, min=-reach, max=reach).astype(kind)


def setup_inputs(seed: int = 0) -> dict:
    splits = jax.random.split(jax.random.key(seed), 6)
    tok_grad = draw_tok_grad(jax.random.fold_in(splits[5], 71), 0)
    expert_ids_keys = jax.random.split(jax.random.fold_in(splits[1], 1), TOKENS // TOK_DEV)
    expert_ids_turns = jax.random.permutation(jax.random.fold_in(splits[1], 3), TOKENS // TOK_DEV)
    expert_ids = jax.vmap(lambda own, number: routed_block(jax.random.fold_in(splits[1], 2), own, number, TOK_DEV, EXP_ALL, TOP, CAP, 2))(expert_ids_keys, expert_ids_turns).reshape((TOKENS, TOP))
    route_probs = jnp.clip(jnp.exp(math.log(1.0) - 2.9996462 * jax.random.uniform(splits[2], (TOKENS, TOP), jnp.float32) ** shard_levels(splits[2], (TOKENS, TOP), ((0, 32),), -0.2, 0.2)), 0.049804688, 1.0).astype(jnp.bfloat16)
    hidden_slots = draw_hidden_slots(jax.random.fold_in(splits[5], 71), 0)
    down_weight = noise(splits[4], (EXPERTS, D, H), H ** -0.5, 0.15625, ((0, 4), (1, 2)))
    return {"tok_grad": tok_grad, "expert_ids": expert_ids, "route_probs": route_probs, "hidden_slots": hidden_slots, "down_weight": down_weight}


clip_level = 40.0


def slot_layout(ids_group):
    expert_iota = jnp.arange(EXPERTS, dtype=jnp.int32)

    def per_source(source, ids_source):
        pairs = ids_source.reshape(-1).astype(jnp.int32)
        onehot = (pairs[:, None] == expert_iota[None, :]).astype(jnp.int32)
        before = jnp.cumsum(onehot, axis=0, dtype=jnp.int32) - onehot
        order = jnp.sum(before * onehot, axis=1, dtype=jnp.int32)
        target = pairs * (N_EXP * CAP) + source * CAP + order
        return jnp.where(pairs < EXPERTS, target, EXPERTS * N_EXP * CAP).astype(jnp.int32)

    sources = jnp.arange(N_EXP, dtype=jnp.int32)
    return jax.vmap(per_source)(sources, ids_group)


def group_work(tok_group, ids_group, probs_group, hidden_group, down_weight):
    target = slot_layout(ids_group.reshape(N_EXP, TOK_DEV, TOP)).reshape(-1)
    total_slots = EXPERTS * N_EXP * CAP
    pair_rows = jnp.repeat(tok_group, TOP, axis=0)
    recv_rows = jnp.zeros((total_slots + 1, D), jnp.bfloat16).at[target].set(pair_rows)
    recv_rows = recv_rows[:total_slots].reshape(EXPERTS, N_EXP * CAP, D)
    recv_probs = jnp.zeros((total_slots + 1,), jnp.bfloat16).at[target].set(probs_group.reshape(-1))
    recv_probs = recv_probs[:total_slots].reshape(EXPERTS, N_EXP * CAP)

    def per_expert(inputs):
        rows_here, probs_here, hidden_here, weight_here = inputs
        scaled = (probs_here.astype(jnp.float32)[:, None] * rows_here.astype(jnp.float32)).astype(jnp.bfloat16)
        outputs = lax.dot_general(hidden_here, weight_here, (((1,), (1,)), ((), ())), preferred_element_type=jnp.float32)
        score = jnp.sum(rows_here.astype(jnp.float32) * outputs, axis=1)
        hidden_grad = jnp.dot(scaled, weight_here, preferred_element_type=jnp.float32).astype(jnp.bfloat16)
        partial_grad = lax.dot_general(scaled, hidden_here, (((0,), (0,)), ((), ())), preferred_element_type=jnp.float32)
        return score, hidden_grad, partial_grad

    score, hidden_grad, partial_grad = lax.map(per_expert, (recv_rows, recv_probs, hidden_group, down_weight))
    flat_scores = jnp.concatenate([score.reshape(-1), jnp.zeros((1,), jnp.float32)])
    route_grad = flat_scores[target].reshape(N_EXP * TOK_DEV, TOP)
    return route_grad, hidden_grad, partial_grad


def reference(tok_grad, expert_ids, route_probs, hidden_slots, down_weight):
    tok_all = tok_grad.reshape(N_REP, N_FSDP, N_EXP * TOK_DEV, D)
    ids_all = expert_ids.reshape(N_REP, N_FSDP, N_EXP * TOK_DEV, TOP)
    probs_all = route_probs.reshape(N_REP, N_FSDP, N_EXP * TOK_DEV, TOP)
    hidden_all = hidden_slots.reshape(N_REP, N_FSDP, EXPERTS, SLOTS, H)

    def replica(inputs):
        def stepper(running, group_inputs):
            tok_group, ids_group, probs_group, hidden_group = group_inputs
            route_grad, hidden_grad, partial_grad = group_work(tok_group, ids_group, probs_group, hidden_group, down_weight)
            return running + partial_grad, (route_grad, hidden_grad)

        start_sum = jnp.zeros((EXPERTS, D, H), jnp.float32)
        summed, outputs = lax.scan(stepper, start_sum, inputs)
        return summed, outputs[0], outputs[1]

    summed, route_grads, hidden_grads = lax.map(replica, (tok_all, ids_all, probs_all, hidden_all))
    peak = jnp.max(jnp.abs(summed), axis=(0, 2, 3))
    factor = jnp.minimum(1.0, clip_level / (peak + 1e-6))
    weight_grad = (summed * factor[None, :, None, None]).astype(jnp.bfloat16)
    return route_grads.reshape(TOKENS, TOP), hidden_grads.reshape(GROUPS, EXPERTS, SLOTS, H), weight_grad
```

```python
import functools

import jax
import jax.numpy as jnp
from jax import lax
from jax.experimental import pallas as pl
from jax.experimental.pallas import tpu as pltpu
from jax.sharding import PartitionSpec as P

clip_level = 40.0
f32 = jnp.float32
bf16 = jnp.bfloat16
VMEM = pltpu.VMEM


def round_up(n, m):
    return (n + m - 1) // m * m


def iota(shape, dim):
    return lax.broadcasted_iota(jnp.int32, shape, dim)


def dot(a, b, dims):
    return lax.dot_general(a, b, (dims, ((), ())), preferred_element_type=f32)


def call(kernel, outs, flops, name, scratch=(), out_specs=None, in_specs=None):
    def run(*args):
        specs = in_specs or [pl.BlockSpec(memory_space=VMEM)] * len(args)
        return pl.pallas_call(
            kernel,
            out_shape=outs,
            in_specs=specs,
            out_specs=out_specs or [pl.BlockSpec(memory_space=VMEM)] * len(outs),
            scratch_shapes=list(scratch),
            compiler_params=pltpu.CompilerParams(vmem_limit_bytes=48 * 1024 * 1024),
            cost_estimate=pl.CostEstimate(flops=flops, bytes_accessed=1 << 20, transcendentals=0),
            name=name,
        )(*args)

    return run


def route_kernel(fsdp, room, ids_ref, probs_ref, tok_ref, send_ref, taken_ref):
    choices, tokens = ids_ref.shape
    slots = taken_ref.shape[0]
    part = tok_ref.shape[0] // fsdp
    width = send_ref.shape[2]
    slot = iota((slots, tokens), 0)
    expert = slot // room
    named = jnp.zeros((slots, tokens), jnp.bool_)
    prob = jnp.zeros((slots, tokens), f32)
    for k in range(choices):
        hit = ids_ref[k : k + 1, :] == expert
        named = named | hit
        prob = jnp.where(hit, probs_ref[k : k + 1, :].astype(f32), prob)
    earlier = (iota((tokens, tokens), 0) < iota((tokens, tokens), 1)).astype(bf16)
    order = dot(jnp.where(named, 1.0, 0.0).astype(bf16), earlier, ((1,), (0,)))
    taken = named & (order == (slot - expert * room).astype(f32))
    picker = jnp.where(taken, 1.0, 0.0)
    taken_ref[...] = picker
    prob = jnp.sum(jnp.where(taken, prob, 0.0), axis=1, keepdims=True)
    lane = iota((slots, width - part), 1)
    tail = jnp.where(lane == 0, prob, 0.0).astype(bf16)
    picker = picker.astype(bf16)
    for f in range(fsdp):
        rows = dot(picker, tok_ref[f * part : (f + 1) * part, :], ((1,), (1,))).astype(bf16)
        block = jnp.concatenate([rows, tail], axis=1)
        count = slots // room
        send_ref[f * count : (f + 1) * count] = block.reshape(count, room, width)


def outputs_kernel(capacity, room, *refs):
    hidden_refs, weight_ref, padded_ref, outputs_ref = refs[:-3], refs[-3], refs[-2], refs[-1]
    fsdp = len(hidden_refs)
    rows = padded_ref.shape[0] // fsdp
    slot_count = hidden_refs[0].shape[0]
    me = lax.axis_index("fsdp")
    to, at = iota((rows, slot_count), 0), iota((rows, slot_count), 1)
    source, order = to // room, to % room
    spread = jnp.where((order < capacity) & (at == source * capacity + order), 1.0, 0.0).astype(bf16)
    for d, ref in enumerate(hidden_refs):
        group = lax.rem(me + fsdp - d, fsdp)
        where = pl.ds(pl.multiple_of(group * rows, rows), rows)
        padded_ref[where, :] = dot(spread, ref[...], ((1,), (0,))).astype(bf16)
    outputs_ref[...] = dot(padded_ref[...], weight_ref[...], ((1,), (1,)))


def summed_kernel(replicas, got_ref, padded_ref, outputs_ref, summed_ref, scaled_ref, pack_ref):
    blocks, room, width = got_ref.shape
    total = blocks * room
    part = outputs_ref.shape[1]
    got = got_ref[...].reshape(total, width)
    rows = got[:, :part].astype(f32)
    prob = got[:, part : part + 1].astype(f32)
    scaled = (prob * rows).astype(bf16)
    scaled_ref[...] = scaled
    summed = dot(scaled, padded_ref[...], ((0,), (0,)))
    summed_ref[...] = summed
    peak = jnp.max(jnp.abs(summed))
    score = jnp.sum(rows * outputs_ref[...], axis=1, keepdims=True)
    lane = iota((total, 128), 1)
    order = iota((total, 128), 0) % room
    spread = jnp.where(lane == order, score, 0.0).reshape(blocks, room, 128)
    packed = jnp.sum(spread, axis=1)
    packed = jnp.where(iota((blocks, 128), 1) == room, peak, packed)
    for r in range(replicas):
        pack_ref[r * blocks : (r + 1) * blocks, 0, :] = packed


def hidden_kernel(capacity, room, scaled_ref, weight_ref, own_ref, *send_refs):
    fsdp = len(send_refs) + 1
    total = scaled_ref.shape[0]
    rows = total // fsdp
    slot_count = own_ref.shape[0]
    me = lax.axis_index("fsdp")
    to, at = iota((slot_count, rows), 0), iota((slot_count, rows), 1)
    pick = jnp.where(at == to // capacity * room + to % capacity, 1.0, 0.0).astype(bf16)
    for d, ref in enumerate((own_ref,) + send_refs):
        group = lax.rem(me + d, fsdp)
        where = pl.ds(pl.multiple_of(group * rows, rows), rows)
        dense = dot(pick, scaled_ref[where, :], ((1,), (0,))).astype(bf16)
        ref[...] = dot(dense, weight_ref[...], ((1,), (0,))).astype(ref.dtype)


def final_kernel(
    experts, fsdp, room, recv_ref, summed_ref, ids_ref, taken_ref, weight_ref, route_ref, held, sems
):
    devices = recv_ref.shape[0]
    blocks = fsdp * experts
    replica, expert = lax.axis_index("rep"), lax.axis_index("exp")
    recv = recv_ref[...].reshape(devices, 128)
    row, lane = iota((devices, 128), 0), iota((devices, 128), 1)
    peak = jnp.max(jnp.where((lane == room) & (row % experts == expert), recv, 0.0))
    factor = jnp.minimum(1.0, clip_level / (jnp.full((1, 1), peak, f32) + 1e-06))
    chunks = sems.shape[0]
    size = summed_ref.shape[0] // chunks
    copies = []
    for c in range(chunks):
        part = slice(c * size, (c + 1) * size)
        held[part, :] = (summed_ref[part, :] * factor).astype(bf16)
        copy = pltpu.make_async_copy(held.at[part, :], weight_ref.at[part, :], sems.at[c])
        copy.start()
        copies.append(copy)
    slots, tokens = taken_ref.shape
    mine = jnp.zeros((experts, 128), f32)
    for f in range(fsdp):
        start = replica * blocks + f * experts
        mine = mine + recv_ref[pl.ds(start, experts), 0, :]
    spread = jnp.broadcast_to(mine[:, None, :], (experts, room, 128)).reshape(slots, 128)
    order = iota((slots, 128), 0) % room
    score = jnp.sum(jnp.where(iota((slots, 128), 1) == order, spread, 0.0), axis=1, keepdims=True)
    slot_expert = iota((slots, tokens), 0) // room
    found = taken_ref[...] * score
    for k in range(ids_ref.shape[0]):
        hit = ids_ref[k : k + 1, :] == slot_expert
        route_ref[k : k + 1, :] = jnp.sum(jnp.where(hit, found, 0.0), axis=0, keepdims=True)
    for copy in copies:
        copy.wait()


def on_device(tok_grad, expert_ids, route_probs, hidden_slots, down_weight):
    experts, fsdp, replicas = lax.axis_size("exp"), lax.axis_size("fsdp"), lax.axis_size("rep")
    slot_count, width = hidden_slots.shape[2:]
    capacity = slot_count // experts
    room = round_up(capacity, 8)
    tokens, features = tok_grad.shape
    choices = expert_ids.shape[1]
    part = down_weight.shape[1]
    padded = round_up(part + 1, 128)
    blocks, slots = fsdp * experts, experts * room
    total = blocks * room
    devices = replicas * blocks
    shape = jax.ShapeDtypeStruct
    hidden, weight = hidden_slots[0, 0], down_weight[0]
    ids = expert_ids.T

    def ring(d):
        return [(i, (i + d) % fsdp) for i in range(fsdp)]

    send, taken = call(
        functools.partial(route_kernel, fsdp, room),
        [shape((blocks, room, padded), bf16), shape((slots, tokens), f32)],
        2 * slots * tokens * features,
        "route",
    )(ids, route_probs.T, tok_grad.T)
    got = lax.all_to_all(send, ("fsdp", "exp"), split_axis=0, concat_axis=0, tiled=True)
    hiddens = [hidden] + [lax.ppermute(hidden, "fsdp", ring(d)) for d in range(1, fsdp)]
    hidden_padded, outputs = call(
        functools.partial(outputs_kernel, capacity, room),
        [shape((total, width), bf16), shape((total, part), f32)],
        2 * total * part * width,
        "outputs",
    )(*hiddens, weight)
    summed, scaled, pack = call(
        functools.partial(summed_kernel, replicas),
        [shape((part, width), f32), shape((total, part), bf16), shape((devices, 1, 128), f32)],
        2 * total * part * width,
        "summed",
    )(got, hidden_padded, outputs)
    recv = lax.all_to_all(pack, ("rep", "fsdp", "exp"), split_axis=0, concat_axis=0, tiled=True)
    own, *others = call(
        functools.partial(hidden_kernel, capacity, room),
        [shape((slot_count, width), f32)] + [shape((slot_count, width), bf16)] * (fsdp - 1),
        2 * total * part * width,
        "hidden",
    )(scaled, weight)
    hidden_acc = own
    for d in range(1, fsdp):
        hidden_acc = hidden_acc + lax.ppermute(others[d - 1], "fsdp", ring(d)).astype(f32)
    hidden_grad = hidden_acc.astype(bf16).reshape(1, 1, slot_count, width)
    sizes = [c for c in range(16, 161, 16) if part % c == 0] or [part]
    chunks = part // sizes[-1]
    weight_grad, route_grad = call(
        functools.partial(final_kernel, experts, fsdp, room),
        [shape((part, width), bf16), shape((choices, tokens), f32)],
        part * width,
        "final",
        scratch=[VMEM((part, width), bf16), pltpu.SemaphoreType.DMA((chunks,))],
        out_specs=[pl.BlockSpec(memory_space=pl.ANY), pl.BlockSpec(memory_space=VMEM)],
    )(recv, summed, ids, taken)
    return route_grad.T, hidden_grad, weight_grad.reshape(1, 1, part, width)


def solution(mesh):
    placed = (
        P(("rep", "fsdp", "exp"), None),
        P(("rep", "fsdp", "exp"), None),
        P(("rep", "fsdp", "exp"), None),
        P(("rep", "fsdp"), "exp", None, None),
        P("exp", "fsdp", None),
    )
    return jax.shard_map(
        on_device,
        mesh=mesh,
        in_specs=placed,
        out_specs=(
            P(("rep", "fsdp", "exp"), None),
            P(("rep", "fsdp"), "exp", None, None),
            P("rep", "exp", "fsdp", None),
        ),
        check_vma=False,
    )
```

```python
import functools

import jax
import jax.numpy as jnp
from jax import lax
from jax.experimental import pallas as pl
from jax.experimental.pallas import tpu as pltpu
from jax.sharding import PartitionSpec as P


clip_level = 40.0
f32 = jnp.float32
bf16 = jnp.bfloat16
VMEM = pltpu.VMEM


def round_up(n, m):
    return (n + m - 1) // m * m


def iota(shape, dim):
    return lax.broadcasted_iota(jnp.int32, shape, dim)


def dot(a, b, dims):
    return lax.dot_general(a, b, (dims, ((), ())), preferred_element_type=f32)


def call(kernel, outs, flops, scratch=(), out_specs=None, in_specs=None):
    def run(*args):
        specs = in_specs or [pl.BlockSpec(memory_space=VMEM)] * len(args)
        return pl.pallas_call(
            kernel,
            out_shape=outs,
            in_specs=specs,
            out_specs=out_specs or [pl.BlockSpec(memory_space=VMEM)] * len(outs),
            scratch_shapes=list(scratch),
            compiler_params=pltpu.CompilerParams(vmem_limit_bytes=24 * 1024 * 1024),
            cost_estimate=pl.CostEstimate(flops=flops, bytes_accessed=1 << 20, transcendentals=0),
        )(*args)

    return run


def route_kernel(
    fsdp, room, ids_in, probs_in, tok_in, hidden_in, send_ref, taken_ref, hidden_ref, ids_ref, probs_ref, tok_ref, sems
):
    loads = [
        pltpu.make_async_copy(src, dst, sems.at[i])
        for i, (src, dst) in enumerate(
            ((ids_in, ids_ref), (probs_in, probs_ref), (tok_in, tok_ref), (hidden_in, hidden_ref))
        )
    ]
    for load in loads:
        load.start()
    loads[0].wait()
    loads[1].wait()
    choices, tokens = ids_ref.shape
    slots = taken_ref.shape[0]
    part = tok_ref.shape[0] // fsdp
    width = send_ref.shape[2]
    slot = iota((slots, tokens), 0)
    expert = slot // room
    named = jnp.zeros((slots, tokens), jnp.bool_)
    prob = jnp.zeros((slots, tokens), f32)
    for k in range(choices):
        hit = ids_ref[k : k + 1, :] == expert
        named = named | hit
        prob = jnp.where(hit, probs_ref[k : k + 1, :].astype(f32), prob)
    earlier = (iota((tokens, tokens), 0) < iota((tokens, tokens), 1)).astype(bf16)
    order = dot(jnp.where(named, 1.0, 0.0).astype(bf16), earlier, ((1,), (0,)))
    taken = named & (order == (slot - expert * room).astype(f32))
    picker = jnp.where(taken, 1.0, 0.0)
    taken_ref[...] = picker
    prob = jnp.sum(jnp.where(taken, prob, 0.0), axis=1, keepdims=True)
    lane = iota((slots, width - part), 1)
    tail = jnp.where(lane == 0, prob, 0.0).astype(bf16)
    picker = picker.astype(bf16)
    loads[2].wait()
    for f in range(fsdp):
        rows = dot(picker, tok_ref[f * part : (f + 1) * part, :], ((1,), (1,))).astype(bf16)
        block = jnp.concatenate([rows, tail], axis=1)
        count = slots // room
        send_ref[f * count : (f + 1) * count] = block.reshape(count, room, width)
    loads[3].wait()


def spread_rows(capacity, room, hidden, rows):
    slot_count = hidden.shape[0]
    to, at = iota((rows, slot_count), 0), iota((rows, slot_count), 1)
    source, order = to // room, to % room
    spread = jnp.where((order < capacity) & (at == source * capacity + order), 1.0, 0.0).astype(bf16)
    return dot(spread, hidden, ((1,), (0,))).astype(bf16)


def own_kernel(capacity, room, hidden_ref, weight_in, padded_ref, outputs_ref, weight_ref, sems):
    chunks = sems.shape[0]
    size = weight_in.shape[0] // chunks
    copies = []
    for c in range(chunks):
        part = slice(c * size, (c + 1) * size)
        copy = pltpu.make_async_copy(weight_in.at[part, :], weight_ref.at[part, :], sems.at[c])
        copy.start()
        copies.append(copy)
    padded = spread_rows(capacity, room, hidden_ref[...], padded_ref.shape[0])
    padded_ref[...] = padded
    for copy in copies:
        copy.wait()
    outputs_ref[...] = dot(padded, weight_ref[...], ((1,), (1,)))


def others_kernel(capacity, room, *refs):
    fsdp = (len(refs) - 5) + 1
    own_padded, own_outputs, weight_ref = refs[:3]
    hidden_refs = refs[3:-2]
    padded_ref, outputs_ref = refs[-2:]
    rows = own_padded.shape[0]
    me = lax.axis_index("fsdp")
    for d in range(fsdp):
        group = lax.rem(me + fsdp - d, fsdp)
        where = pl.ds(pl.multiple_of(group * rows, rows), rows)
        if d == 0:
            padded_ref[where, :] = own_padded[...]
            outputs_ref[where, :] = own_outputs[...]
        else:
            padded = spread_rows(capacity, room, hidden_refs[d - 1][...], rows)
            padded_ref[where, :] = padded
            outputs_ref[where, :] = dot(padded, weight_ref[...], ((1,), (1,)))


def summed_kernel(replicas, got_ref, padded_ref, outputs_ref, scaled_ref, pack_ref):
    blocks, room, width = got_ref.shape
    total = blocks * room
    part = outputs_ref.shape[1]
    got = got_ref[...].reshape(total, width)
    rows = got[:, :part].astype(f32)
    prob = got[:, part : part + 1].astype(f32)
    scaled = (prob * rows).astype(bf16)
    scaled_ref[...] = scaled
    peak = jnp.max(jnp.abs(dot(scaled, padded_ref[...], ((0,), (0,)))))
    score = jnp.sum(rows * outputs_ref[...], axis=1, keepdims=True)
    lane = iota((total, 128), 1)
    order = iota((total, 128), 0) % room
    spread = jnp.where(lane == order, score, 0.0).reshape(blocks, room, 128)
    packed = jnp.sum(spread, axis=1)
    packed = jnp.where(iota((blocks, 128), 1) == room, peak, packed)
    for r in range(replicas):
        pack_ref[r * blocks : (r + 1) * blocks, 0, :] = packed


def hidden_kernel(capacity, room, scaled_ref, weight_ref, turned_ref, own_ref, *send_refs):
    fsdp = len(send_refs) + 1
    total = scaled_ref.shape[0]
    rows = total // fsdp
    slot_count = own_ref.shape[0]
    me = lax.axis_index("fsdp")
    to, at = iota((slot_count, rows), 0), iota((slot_count, rows), 1)
    pick = jnp.where(at == to // capacity * room + to % capacity, 1.0, 0.0).astype(bf16)
    for d, ref in enumerate((own_ref,) + send_refs):
        group = lax.rem(me + d, fsdp)
        where = pl.ds(pl.multiple_of(group * rows, rows), rows)
        dense = dot(pick, scaled_ref[where, :], ((1,), (0,))).astype(bf16)
        ref[...] = dot(dense, weight_ref[...], ((1,), (0,))).astype(ref.dtype)
    turned_ref[...] = scaled_ref[...].T


def final_kernel(experts, fsdp, room, recv_ref, turned_ref, padded_ref, ids_ref, taken_ref, own_ref, *refs):
    other_refs = refs[: fsdp - 1]
    weight_ref, route_ref, hidden_ref, held, sems = refs[fsdp - 1 :]
    devices = recv_ref.shape[0]
    blocks = fsdp * experts
    replica, expert = lax.axis_index("rep"), lax.axis_index("exp")
    recv = recv_ref[...].reshape(devices, 128)
    row, lane = iota((devices, 128), 0), iota((devices, 128), 1)
    peak = jnp.max(jnp.where((lane == room) & (row % experts == expert), recv, 0.0))
    factor = jnp.minimum(1.0, clip_level / (jnp.full((1, 1), peak, f32) + 1e-06))
    chunks = sems.shape[0]
    size = turned_ref.shape[0] // chunks
    copies = []
    for c in range(chunks):
        part = slice(c * size, (c + 1) * size)
        summed = dot(turned_ref[part, :], padded_ref[...], ((1,), (0,)))
        held[part, :] = (summed * factor).astype(bf16)
        copy = pltpu.make_async_copy(held.at[part, :], weight_ref.at[part, :], sems.at[c])
        copy.start()
        copies.append(copy)
    slots, tokens = taken_ref.shape
    mine = jnp.zeros((experts, 128), f32)
    for f in range(fsdp):
        start = replica * blocks + f * experts
        mine = mine + recv_ref[pl.ds(start, experts), 0, :]
    spread = jnp.broadcast_to(mine[:, None, :], (experts, room, 128)).reshape(slots, 128)
    order = iota((slots, 128), 0) % room
    score = jnp.sum(jnp.where(iota((slots, 128), 1) == order, spread, 0.0), axis=1, keepdims=True)
    slot_expert = iota((slots, tokens), 0) // room
    found = taken_ref[...] * score
    for k in range(ids_ref.shape[0]):
        hit = ids_ref[k : k + 1, :] == slot_expert
        route_ref[k : k + 1, :] = jnp.sum(jnp.where(hit, found, 0.0), axis=0, keepdims=True)
    total = own_ref[...]
    for ref in other_refs:
        total = total + ref[...].astype(f32)
    hidden_ref[...] = total.astype(bf16)
    for copy in copies:
        copy.wait()


def on_device(tok_grad, expert_ids, route_probs, hidden_slots, down_weight):
    experts, fsdp, replicas = lax.axis_size("exp"), lax.axis_size("fsdp"), lax.axis_size("rep")
    slot_count, width = hidden_slots.shape[2:]
    capacity = slot_count // experts
    room = round_up(capacity, 8)
    tokens, features = tok_grad.shape
    choices = expert_ids.shape[1]
    part = down_weight.shape[1]
    padded = round_up(part + 1, 128)
    blocks, slots = fsdp * experts, experts * room
    total = blocks * room
    devices = replicas * blocks
    shape = jax.ShapeDtypeStruct
    hidden, weight = hidden_slots[0, 0], down_weight[0]
    ids = expert_ids.T

    def ring(d):
        return [(i, (i + d) % fsdp) for i in range(fsdp)]

    any_space, vmem = pl.BlockSpec(memory_space=pl.ANY), pl.BlockSpec(memory_space=VMEM)

    def stay(x):
        return pltpu.with_memory_space_constraint(x, pltpu.HBM)

    sizes = [c for c in range(8, 161, 8) if part % c == 0] or [part]
    chunks = part // sizes[-1]
    send, taken, hidden = call(
        functools.partial(route_kernel, fsdp, room),
        [shape((blocks, room, padded), bf16), shape((slots, tokens), f32), shape((slot_count, width), bf16)],
        2 * slots * tokens * features,
        in_specs=[any_space] * 4,
        scratch=[
            VMEM((choices, tokens), jnp.int32),
            VMEM((choices, tokens), bf16),
            VMEM((features, tokens), bf16),
            pltpu.SemaphoreType.DMA((4,)),
        ],
    )(stay(ids), stay(route_probs.T), stay(tok_grad.T), stay(hidden))
    got = lax.all_to_all(send, ("fsdp", "exp"), split_axis=0, concat_axis=0, tiled=True)
    others = [lax.ppermute(hidden_slots[0, 0], "fsdp", ring(d)) for d in range(1, fsdp)]
    own_padded, own_outputs, weight = call(
        functools.partial(own_kernel, capacity, room),
        [shape((slots, width), bf16), shape((slots, part), f32), shape((part, width), bf16)],
        2 * total * part * width,
        in_specs=[vmem, any_space],
        scratch=[pltpu.SemaphoreType.DMA((chunks,))],
    )(hidden, stay(weight))
    hidden_padded, outputs = call(
        functools.partial(others_kernel, capacity, room),
        [shape((total, width), bf16), shape((total, part), f32)],
        2 * total * part * width,
    )(own_padded, own_outputs, weight, *others)
    scaled, pack = call(
        functools.partial(summed_kernel, replicas),
        [shape((total, part), bf16), shape((devices, 1, 128), f32)],
        2 * total * part * width,
    )(got, hidden_padded, outputs)
    recv = lax.all_to_all(pack, ("rep", "fsdp", "exp"), split_axis=0, concat_axis=0, tiled=True)
    turned, own, *sends = call(
        functools.partial(hidden_kernel, capacity, room),
        [shape((part, total), bf16), shape((slot_count, width), f32)]
        + [shape((slot_count, width), bf16)] * (fsdp - 1),
        2 * total * part * width,
    )(scaled, weight)
    parts = [lax.ppermute(sends[d - 1], "fsdp", ring(d)) for d in range(1, fsdp)]
    weight_grad, route_grad, hidden_grad = call(
        functools.partial(final_kernel, experts, fsdp, room),
        [shape((part, width), bf16), shape((choices, tokens), f32), shape((slot_count, width), bf16)],
        part * width,
        scratch=[VMEM((part, width), bf16), pltpu.SemaphoreType.DMA((chunks,))],
        out_specs=[any_space, vmem, vmem],
    )(recv, turned, hidden_padded, ids, taken, own, *parts)
    return route_grad.T, hidden_grad[None, None], weight_grad.reshape(1, 1, part, width)


def solution(mesh):
    placed = (
        P(("rep", "fsdp", "exp"), None),
        P(("rep", "fsdp", "exp"), None),
        P(("rep", "fsdp", "exp"), None),
        P(("rep", "fsdp"), "exp", None, None),
        P("exp", "fsdp", None),
    )

    return jax.shard_map(
        on_device,
        mesh=mesh,
        in_specs=placed,
        out_specs=(
            P(("rep", "fsdp", "exp"), None),
            P(("rep", "fsdp"), "exp", None, None),
            P("rep", "exp", "fsdp", None),
        ),
        check_vma=False,
    )
```

```python
import functools

import jax
import jax.numpy as jnp
from jax import lax
from jax.experimental import pallas as pl
from jax.experimental.pallas import tpu as pltpu
from jax.sharding import PartitionSpec as P


clip_level = 40.0
f32 = jnp.float32
bf16 = jnp.bfloat16
VMEM = pltpu.VMEM


def round_up(n, m):
    return (n + m - 1) // m * m


def iota(shape, dim):
    return lax.broadcasted_iota(jnp.int32, shape, dim)


def dot(a, b, dims):
    return lax.dot_general(a, b, (dims, ((), ())), preferred_element_type=f32)


def call(kernel, outs, flops, scratch=(), out_specs=None, in_specs=None):
    def run(*args):
        specs = in_specs or [pl.BlockSpec(memory_space=VMEM)] * len(args)
        return pl.pallas_call(
            kernel,
            out_shape=outs,
            in_specs=specs,
            out_specs=out_specs or [pl.BlockSpec(memory_space=VMEM)] * len(outs),
            scratch_shapes=list(scratch),
            compiler_params=pltpu.CompilerParams(vmem_limit_bytes=24 * 1024 * 1024),
            cost_estimate=pl.CostEstimate(flops=flops, bytes_accessed=1 << 20, transcendentals=0),
        )(*args)

    return run


def route_kernel(
    fsdp, room, ids_in, probs_in, tok_in, send_ref, taken_ref, ids_ref, probs_ref, tok_ref, held, sems, out_sems
):
    loads = [
        pltpu.make_async_copy(src, dst, sems.at[i])
        for i, (src, dst) in enumerate(
            ((ids_in, ids_ref), (probs_in, probs_ref), (tok_in, tok_ref))
        )
    ]
    for load in loads:
        load.start()
    loads[0].wait()
    loads[1].wait()
    choices, tokens = ids_ref.shape
    slots = taken_ref.shape[0]
    part = tok_ref.shape[0] // fsdp
    width = send_ref.shape[2]
    slot = iota((slots, tokens), 0)
    expert = slot // room
    named = jnp.zeros((slots, tokens), jnp.bool_)
    prob = jnp.zeros((slots, tokens), f32)
    for k in range(choices):
        hit = ids_ref[k : k + 1, :] == expert
        named = named | hit
        prob = jnp.where(hit, probs_ref[k : k + 1, :].astype(f32), prob)
    earlier = (iota((tokens, tokens), 0) < iota((tokens, tokens), 1)).astype(bf16)
    order = dot(jnp.where(named, 1.0, 0.0).astype(bf16), earlier, ((1,), (0,)))
    taken = named & (order == (slot - expert * room).astype(f32))
    picker = jnp.where(taken, 1.0, 0.0)
    taken_ref[...] = picker
    prob = jnp.sum(jnp.where(taken, prob, 0.0), axis=1, keepdims=True)
    lane = iota((slots, width - part), 1)
    tail = jnp.where(lane == 0, prob, 0.0).astype(bf16)
    picker = picker.astype(bf16)
    loads[2].wait()
    stores = []
    for f in range(fsdp):
        rows = dot(picker, tok_ref[f * part : (f + 1) * part, :], ((1,), (1,))).astype(bf16)
        block = jnp.concatenate([rows, tail], axis=1)
        count = slots // room
        where = slice(f * count, (f + 1) * count)
        held[where] = block.reshape(count, room, width)
        store = pltpu.make_async_copy(held.at[where], send_ref.at[where], out_sems.at[f])
        store.start()
        stores.append(store)
    for store in stores:
        store.wait()


def spread_rows(capacity, room, hidden, rows):
    slot_count = hidden.shape[0]
    to, at = iota((rows, slot_count), 0), iota((rows, slot_count), 1)
    source, order = to // room, to % room
    spread = jnp.where((order < capacity) & (at == source * capacity + order), 1.0, 0.0).astype(bf16)
    return dot(spread, hidden, ((1,), (0,))).astype(bf16)


def outputs_kernel(capacity, room, fsdp, own_in, weight_in, *refs):
    other_refs = refs[: fsdp - 1]
    padded_ref, outputs_ref, weight_ref, own_ref, own_sem, sems = refs[fsdp - 1 :]
    part = weight_in.shape[0]
    rows = padded_ref.shape[0] // fsdp
    chunks = sems.shape[0]
    size = round_up(-(-part // chunks), 128)
    own = pltpu.make_async_copy(own_in, own_ref, own_sem)
    own.start()
    copies = []
    for c in range(chunks):
        where = slice(c * size, min((c + 1) * size, part))
        copy = pltpu.make_async_copy(weight_in.at[where, :], weight_ref.at[where, :], sems.at[c])
        copy.start()
        copies.append((where, copy))
    me = lax.axis_index("fsdp")
    own.wait()
    for d, ref in enumerate((own_ref,) + other_refs):
        group = lax.rem(me + fsdp - d, fsdp)
        to = pl.ds(pl.multiple_of(group * rows, rows), rows)
        padded_ref[to, :] = spread_rows(capacity, room, ref[...], rows)
    padded = padded_ref[...]
    for where, copy in copies:
        copy.wait()
        outputs_ref[:, where] = dot(padded, weight_ref[where, :], ((1,), (1,)))


def summed_kernel(replicas, got_ref, padded_ref, outputs_ref, scaled_ref, pack_ref):
    blocks, room, width = got_ref.shape
    total = blocks * room
    part = outputs_ref.shape[1]
    got = got_ref[...].reshape(total, width)
    rows = got[:, :part].astype(f32)
    prob = got[:, part : part + 1].astype(f32)
    scaled = (prob * rows).astype(bf16)
    scaled_ref[...] = scaled
    peak = jnp.max(jnp.abs(dot(scaled, padded_ref[...], ((0,), (0,)))))
    score = jnp.sum(rows * outputs_ref[...], axis=1, keepdims=True)
    lane = iota((total, 128), 1)
    order = iota((total, 128), 0) % room
    spread = jnp.where(lane == order, score, 0.0).reshape(blocks, room, 128)
    packed = jnp.sum(spread, axis=1)
    packed = jnp.where(iota((blocks, 128), 1) == room, peak, packed)
    for r in range(replicas):
        pack_ref[r * blocks : (r + 1) * blocks, 0, :] = packed


def hidden_kernel(capacity, room, scaled_ref, weight_ref, turned_ref, own_ref, *send_refs):
    fsdp = len(send_refs) + 1
    total = scaled_ref.shape[0]
    rows = total // fsdp
    slot_count = own_ref.shape[0]
    me = lax.axis_index("fsdp")
    to, at = iota((slot_count, rows), 0), iota((slot_count, rows), 1)
    pick = jnp.where(at == to // capacity * room + to % capacity, 1.0, 0.0).astype(bf16)
    for d, ref in enumerate((own_ref,) + send_refs):
        group = lax.rem(me + d, fsdp)
        where = pl.ds(pl.multiple_of(group * rows, rows), rows)
        dense = dot(pick, scaled_ref[where, :], ((1,), (0,))).astype(bf16)
        ref[...] = dot(dense, weight_ref[...], ((1,), (0,))).astype(ref.dtype)
    turned_ref[...] = scaled_ref[...].T


def final_kernel(experts, fsdp, room, recv_ref, turned_ref, padded_ref, ids_ref, taken_ref, own_ref, *refs):
    other_refs = refs[: fsdp - 1]
    weight_ref, route_out, hidden_out, held, route_ref, hidden_ref, sems, small_sems = refs[fsdp - 1 :]
    devices = recv_ref.shape[0]
    blocks = fsdp * experts
    replica, expert = lax.axis_index("rep"), lax.axis_index("exp")
    recv = recv_ref[...].reshape(devices, 128)
    row, lane = iota((devices, 128), 0), iota((devices, 128), 1)
    peak = jnp.max(jnp.where((lane == room) & (row % experts == expert), recv, 0.0))
    factor = jnp.minimum(1.0, clip_level / (jnp.full((1, 1), peak, f32) + 1e-06))
    chunks = sems.shape[0]
    size = turned_ref.shape[0] // chunks
    copies = []
    for c in range(chunks):
        part = slice(c * size, (c + 1) * size)
        summed = dot(turned_ref[part, :], padded_ref[...], ((1,), (0,)))
        held[part, :] = (summed * factor).astype(bf16)
        copy = pltpu.make_async_copy(held.at[part, :], weight_ref.at[part, :], sems.at[c])
        copy.start()
        copies.append(copy)
    slots, tokens = taken_ref.shape
    mine = jnp.zeros((experts, 128), f32)
    for f in range(fsdp):
        start = replica * blocks + f * experts
        mine = mine + recv_ref[pl.ds(start, experts), 0, :]
    spread = jnp.broadcast_to(mine[:, None, :], (experts, room, 128)).reshape(slots, 128)
    order = iota((slots, 128), 0) % room
    score = jnp.sum(jnp.where(iota((slots, 128), 1) == order, spread, 0.0), axis=1, keepdims=True)
    slot_expert = iota((slots, tokens), 0) // room
    found = taken_ref[...] * score
    for k in range(ids_ref.shape[0]):
        hit = ids_ref[k : k + 1, :] == slot_expert
        route_ref[k : k + 1, :] = jnp.sum(jnp.where(hit, found, 0.0), axis=0, keepdims=True)
    copies.append(pltpu.make_async_copy(route_ref, route_out, small_sems.at[0]))
    copies[-1].start()
    total = own_ref[...]
    for ref in other_refs:
        total = total + ref[...].astype(f32)
    hidden_ref[...] = total.astype(bf16)
    copies.append(pltpu.make_async_copy(hidden_ref, hidden_out, small_sems.at[1]))
    copies[-1].start()
    for copy in copies:
        copy.wait()


def on_device(tok_grad, expert_ids, route_probs, hidden_slots, down_weight):
    experts, fsdp, replicas = lax.axis_size("exp"), lax.axis_size("fsdp"), lax.axis_size("rep")
    slot_count, width = hidden_slots.shape[2:]
    capacity = slot_count // experts
    room = round_up(capacity, 8)
    tokens, features = tok_grad.shape
    choices = expert_ids.shape[1]
    part = down_weight.shape[1]
    padded = round_up(part + 1, 128)
    blocks, slots = fsdp * experts, experts * room
    total = blocks * room
    devices = replicas * blocks
    shape = jax.ShapeDtypeStruct
    hidden, weight = hidden_slots[0, 0], down_weight[0]
    ids = expert_ids.T

    def ring(d):
        return [(i, (i + d) % fsdp) for i in range(fsdp)]

    any_space, vmem = pl.BlockSpec(memory_space=pl.ANY), pl.BlockSpec(memory_space=VMEM)

    def stay(x):
        return pltpu.with_memory_space_constraint(x, pltpu.HBM)

    sizes = [c for c in range(8, 161, 8) if part % c == 0] or [part]
    chunks = part // sizes[-1]
    send, taken = call(
        functools.partial(route_kernel, fsdp, room),
        [pltpu.HBM((blocks, room, padded), bf16), shape((slots, tokens), f32)],
        2 * slots * tokens * features,
        in_specs=[any_space] * 3,
        out_specs=[any_space, vmem],
        scratch=[
            VMEM((choices, tokens), jnp.int32),
            VMEM((choices, tokens), bf16),
            VMEM((features, tokens), bf16),
            VMEM((blocks, room, padded), bf16),
            pltpu.SemaphoreType.DMA((3,)),
            pltpu.SemaphoreType.DMA((fsdp,)),
        ],
    )(stay(ids), stay(route_probs.T), stay(tok_grad.T))
    got = lax.all_to_all(send, ("fsdp", "exp"), split_axis=0, concat_axis=0, tiled=True)
    others = [lax.ppermute(hidden, "fsdp", ring(d)) for d in range(1, fsdp)]
    weight_chunks = -(-part // 256)
    hidden_padded, outputs, weight = call(
        functools.partial(outputs_kernel, capacity, room, fsdp),
        [shape((total, width), bf16), shape((total, part), f32), shape((part, width), bf16)],
        2 * total * part * width,
        in_specs=[any_space] * 2 + [vmem] * (fsdp - 1),
        scratch=[
            VMEM((slot_count, width), bf16),
            pltpu.SemaphoreType.DMA,
            pltpu.SemaphoreType.DMA((weight_chunks,)),
        ],
    )(stay(hidden), stay(weight), *others)
    scaled, pack = call(
        functools.partial(summed_kernel, replicas),
        [shape((total, part), bf16), shape((devices, 1, 128), f32)],
        2 * total * part * width,
    )(got, hidden_padded, outputs)
    recv = lax.all_to_all(pack, ("rep", "fsdp", "exp"), split_axis=0, concat_axis=0, tiled=True)
    turned, own, *sends = call(
        functools.partial(hidden_kernel, capacity, room),
        [shape((part, total), bf16), shape((slot_count, width), f32)]
        + [shape((slot_count, width), bf16)] * (fsdp - 1),
        2 * total * part * width,
    )(scaled, weight)
    parts = [lax.ppermute(sends[d - 1], "fsdp", ring(d)) for d in range(1, fsdp)]
    weight_grad, route_grad, hidden_grad = call(
        functools.partial(final_kernel, experts, fsdp, room),
        [
            pltpu.HBM((part, width), bf16),
            pltpu.HBM((choices, tokens), f32),
            pltpu.HBM((slot_count, width), bf16),
        ],
        part * width,
        scratch=[
            VMEM((part, width), bf16),
            VMEM((choices, tokens), f32),
            VMEM((slot_count, width), bf16),
            pltpu.SemaphoreType.DMA((chunks,)),
            pltpu.SemaphoreType.DMA((2,)),
        ],
        out_specs=[any_space] * 3,
    )(recv, turned, hidden_padded, ids, taken, own, *parts)
    return route_grad.T, hidden_grad[None, None], weight_grad.reshape(1, 1, part, width)


def solution(mesh):
    placed = (
        P(("rep", "fsdp", "exp"), None),
        P(("rep", "fsdp", "exp"), None),
        P(("rep", "fsdp", "exp"), None),
        P(("rep", "fsdp"), "exp", None, None),
        P("exp", "fsdp", None),
    )

    return jax.shard_map(
        on_device,
        mesh=mesh,
        in_specs=placed,
        out_specs=(
            P(("rep", "fsdp", "exp"), None),
            P(("rep", "fsdp"), "exp", None, None),
            P("rep", "exp", "fsdp", None),
        ),
        check_vma=False,
    )
```

```python
import functools

import jax
import jax.numpy as jnp
from jax import lax
from jax.experimental import pallas as pl
from jax.experimental.pallas import tpu as pltpu
from jax.sharding import PartitionSpec as P


clip_level = 40.0
f32 = jnp.float32
bf16 = jnp.bfloat16
VMEM = pltpu.VMEM


def round_up(n, m):
    return (n + m - 1) // m * m


def iota(shape, dim):
    return lax.broadcasted_iota(jnp.int32, shape, dim)


def dot(a, b, dims):
    return lax.dot_general(a, b, (dims, ((), ())), preferred_element_type=f32)


def call(kernel, outs, flops, scratch=(), out_specs=None, in_specs=None):
    def run(*args):
        specs = in_specs or [pl.BlockSpec(memory_space=VMEM)] * len(args)
        return pl.pallas_call(
            kernel,
            out_shape=outs,
            in_specs=specs,
            out_specs=out_specs or [pl.BlockSpec(memory_space=VMEM)] * len(outs),
            scratch_shapes=list(scratch),
            compiler_params=pltpu.CompilerParams(vmem_limit_bytes=24 * 1024 * 1024),
            cost_estimate=pl.CostEstimate(flops=flops, bytes_accessed=1 << 20, transcendentals=0),
        )(*args)

    return run


def route_kernel(
    fsdp, room, lead, ids_in, probs_in, tok_in, send_ref, taken_ref, ids_ref, probs_ref, tok_ref, held, sems, out_sems
):
    loads = [
        pltpu.make_async_copy(src, dst, sems.at[i])
        for i, (src, dst) in enumerate(
            ((ids_in, ids_ref), (probs_in, probs_ref), (tok_in, tok_ref))
        )
    ]
    for load in loads:
        load.start()
    loads[0].wait()
    loads[1].wait()
    choices, tokens = ids_ref.shape
    slots = taken_ref.shape[0]
    part = tok_ref.shape[0] // fsdp
    width = send_ref.shape[2]
    slot = iota((slots, tokens), 0)
    expert = slot // room
    named = jnp.zeros((slots, tokens), jnp.bool_)
    prob = jnp.zeros((slots, tokens), f32)
    for k in range(choices):
        hit = ids_ref[k : k + 1, :] == expert
        named = named | hit
        prob = jnp.where(hit, probs_ref[k : k + 1, :].astype(f32), prob)
    earlier = (iota((tokens, tokens), 0) < iota((tokens, tokens), 1)).astype(bf16)
    order = dot(jnp.where(named, 1.0, 0.0).astype(bf16), earlier, ((1,), (0,)))
    taken = named & (order == (slot - expert * room).astype(f32))
    picker = jnp.where(taken, 1.0, 0.0)
    taken_ref[...] = picker
    prob = jnp.sum(jnp.where(taken, prob, 0.0), axis=1, keepdims=True)
    lane = iota((slots, width - part), 1)
    tail = jnp.where(lane == 0, prob, 0.0).astype(bf16)
    picker = picker.astype(bf16)
    loads[2].wait()
    stores = []
    for f in range(fsdp):
        rows = dot(picker, tok_ref[f * part : (f + 1) * part, :], ((1,), (1,))).astype(bf16)
        block = jnp.concatenate([rows, tail], axis=1)
        count = slots // room
        where = slice(f * count, (f + 1) * count)
        held[where] = block.reshape(count, room, width)
        if f == 0 and lead > 0:
            held[0] = block[lead * room : (lead + 1) * room]
            held[lead] = block[:room]
        store = pltpu.make_async_copy(held.at[where], send_ref.at[where], out_sems.at[f])
        store.start()
        stores.append(store)
    for store in stores:
        store.wait()


def spread_rows(capacity, room, hidden, rows):
    slot_count = hidden.shape[0]
    to, at = iota((rows, slot_count), 0), iota((rows, slot_count), 1)
    source, order = to // room, to % room
    spread = jnp.where((order < capacity) & (at == source * capacity + order), 1.0, 0.0).astype(bf16)
    return dot(spread, hidden, ((1,), (0,))).astype(bf16)


def outputs_kernel(capacity, room, fsdp, own_in, weight_in, *refs):
    other_refs = refs[: fsdp - 1]
    padded_ref, outputs_ref, weight_ref, own_ref, own_sem, sems = refs[fsdp - 1 :]
    part = weight_in.shape[0]
    rows = padded_ref.shape[0] // fsdp
    chunks = sems.shape[0]
    size = round_up(-(-part // chunks), 128)
    own = pltpu.make_async_copy(own_in, own_ref, own_sem)
    own.start()
    copies = []
    for c in range(chunks):
        where = slice(c * size, min((c + 1) * size, part))
        copy = pltpu.make_async_copy(weight_in.at[where, :], weight_ref.at[where, :], sems.at[c])
        copy.start()
        copies.append((where, copy))
    me = lax.axis_index("fsdp")
    own.wait()
    for d, ref in enumerate((own_ref,) + other_refs):
        group = lax.rem(me + fsdp - d, fsdp)
        to = pl.ds(pl.multiple_of(group * rows, rows), rows)
        padded_ref[to, :] = spread_rows(capacity, room, ref[...], rows)
    padded = padded_ref[...]
    for where, copy in copies:
        copy.wait()
    outputs_ref[...] = dot(padded, weight_ref[...], ((1,), (1,)))


def summed_kernel(replicas, lead, got_ref, padded_ref, outputs_ref, scaled_ref, pack_ref):
    blocks, room, width = got_ref.shape
    total = blocks * room
    part = outputs_ref.shape[1]
    got = got_ref[...].reshape(total, width)
    if lead > 0:
        near, far = got[:room], got[lead * room : (lead + 1) * room]
        got = jnp.concatenate([far, got[room : lead * room], near, got[(lead + 1) * room :]], axis=0) if lead > 1 else jnp.concatenate([far, near, got[2 * room :]], axis=0)
    rows = got[:, :part].astype(f32)
    prob = got[:, part : part + 1].astype(f32)
    scaled = (prob * rows).astype(bf16)
    scaled_ref[...] = scaled
    peak = jnp.max(jnp.abs(dot(scaled, padded_ref[...], ((0,), (0,)))))
    score = jnp.sum(rows * outputs_ref[...], axis=1, keepdims=True)
    lane = iota((total, 128), 1)
    order = iota((total, 128), 0) % room
    spread = jnp.where(lane == order, score, 0.0).reshape(blocks, room, 128)
    packed = jnp.sum(spread, axis=1)
    packed = jnp.where(iota((blocks, 128), 1) == room, peak, packed)
    for r in range(replicas):
        pack_ref[r * blocks : (r + 1) * blocks, 0, :] = packed


def hidden_kernel(capacity, room, scaled_ref, weight_ref, turned_ref, own_ref, *send_refs):
    fsdp = len(send_refs) + 1
    total = scaled_ref.shape[0]
    rows = total // fsdp
    slot_count = own_ref.shape[0]
    me = lax.axis_index("fsdp")
    to, at = iota((slot_count, rows), 0), iota((slot_count, rows), 1)
    pick = jnp.where(at == to // capacity * room + to % capacity, 1.0, 0.0).astype(bf16)
    for d, ref in enumerate((own_ref,) + send_refs):
        group = lax.rem(me + d, fsdp)
        where = pl.ds(pl.multiple_of(group * rows, rows), rows)
        dense = dot(pick, scaled_ref[where, :], ((1,), (0,))).astype(bf16)
        ref[...] = dot(dense, weight_ref[...], ((1,), (0,))).astype(ref.dtype)
    turned_ref[...] = scaled_ref[...].T


def final_kernel(experts, fsdp, room, recv_ref, turned_ref, padded_ref, ids_ref, taken_ref, own_ref, *refs):
    other_refs = refs[: fsdp - 1]
    weight_ref, route_out, hidden_out, held, route_ref, hidden_ref, sems, small_sems = refs[fsdp - 1 :]
    devices = recv_ref.shape[0]
    blocks = fsdp * experts
    replica, expert = lax.axis_index("rep"), lax.axis_index("exp")
    recv = recv_ref[...].reshape(devices, 128)
    row, lane = iota((devices, 128), 0), iota((devices, 128), 1)
    peak = jnp.max(jnp.where((lane == room) & (row % experts == expert), recv, 0.0))
    factor = jnp.minimum(1.0, clip_level / (jnp.full((1, 1), peak, f32) + 1e-06))
    chunks = sems.shape[0]
    size = turned_ref.shape[0] // chunks
    copies = []
    for c in range(chunks):
        part = slice(c * size, (c + 1) * size)
        summed = dot(turned_ref[part, :], padded_ref[...], ((1,), (0,)))
        held[part, :] = (summed * factor).astype(bf16)
        copy = pltpu.make_async_copy(held.at[part, :], weight_ref.at[part, :], sems.at[c])
        copy.start()
        copies.append(copy)
    slots, tokens = taken_ref.shape
    mine = jnp.zeros((experts, 128), f32)
    for f in range(fsdp):
        start = replica * blocks + f * experts
        mine = mine + recv_ref[pl.ds(start, experts), 0, :]
    spread = jnp.broadcast_to(mine[:, None, :], (experts, room, 128)).reshape(slots, 128)
    order = iota((slots, 128), 0) % room
    score = jnp.sum(jnp.where(iota((slots, 128), 1) == order, spread, 0.0), axis=1, keepdims=True)
    slot_expert = iota((slots, tokens), 0) // room
    found = taken_ref[...] * score
    for k in range(ids_ref.shape[0]):
        hit = ids_ref[k : k + 1, :] == slot_expert
        route_ref[k : k + 1, :] = jnp.sum(jnp.where(hit, found, 0.0), axis=0, keepdims=True)
    copies.append(pltpu.make_async_copy(route_ref, route_out, small_sems.at[0]))
    copies[-1].start()
    total = own_ref[...]
    for ref in other_refs:
        total = total + ref[...]
    hidden_ref[...] = total.astype(bf16)
    copies.append(pltpu.make_async_copy(hidden_ref, hidden_out, small_sems.at[1]))
    copies[-1].start()
    for copy in copies:
        copy.wait()


def on_device(tok_grad, expert_ids, route_probs, hidden_slots, down_weight):
    experts, fsdp, replicas = lax.axis_size("exp"), lax.axis_size("fsdp"), lax.axis_size("rep")
    slot_count, width = hidden_slots.shape[2:]
    capacity = slot_count // experts
    room = round_up(capacity, 8)
    tokens, features = tok_grad.shape
    choices = expert_ids.shape[1]
    part = down_weight.shape[1]
    padded = round_up(part + 1, 128)
    blocks, slots = fsdp * experts, experts * room
    total = blocks * room
    devices = replicas * blocks
    shape = jax.ShapeDtypeStruct
    hidden, weight = hidden_slots[0, 0], down_weight[0]
    ids = expert_ids.T
    lead = (experts - 1) // 2
    order = list(range(blocks))
    order[0], order[lead] = lead, 0

    def ring(d):
        return [(i, (i + d) % fsdp) for i in range(fsdp)]

    any_space, vmem = pl.BlockSpec(memory_space=pl.ANY), pl.BlockSpec(memory_space=VMEM)

    def stay(x):
        return pltpu.with_memory_space_constraint(x, pltpu.HBM)

    sizes = [c for c in range(8, 161, 8) if part % c == 0] or [part]
    chunks = part // sizes[-1]
    send, taken = call(
        functools.partial(route_kernel, fsdp, room, lead),
        [pltpu.HBM((blocks, room, padded), bf16), shape((slots, tokens), f32)],
        2 * slots * tokens * features,
        in_specs=[any_space] * 3,
        out_specs=[any_space, vmem],
        scratch=[
            VMEM((choices, tokens), jnp.int32),
            VMEM((choices, tokens), bf16),
            VMEM((features, tokens), bf16),
            VMEM((blocks, room, padded), bf16),
            pltpu.SemaphoreType.DMA((3,)),
            pltpu.SemaphoreType.DMA((fsdp,)),
        ],
    )(stay(ids), stay(route_probs.T), stay(tok_grad.T))
    got = lax.all_to_all(
        send,
        ("fsdp", "exp"),
        split_axis=0,
        concat_axis=0,
        axis_index_groups=[order],
        tiled=True,
    )
    others = [lax.ppermute(hidden, "fsdp", ring(d)) for d in range(1, fsdp)]
    weight_chunks = -(-part // 256)
    hidden_padded, outputs, weight = call(
        functools.partial(outputs_kernel, capacity, room, fsdp),
        [shape((total, width), bf16), shape((total, part), f32), shape((part, width), bf16)],
        2 * total * part * width,
        in_specs=[any_space] * 2 + [vmem] * (fsdp - 1),
        scratch=[
            VMEM((slot_count, width), bf16),
            pltpu.SemaphoreType.DMA,
            pltpu.SemaphoreType.DMA((weight_chunks,)),
        ],
    )(stay(hidden), stay(weight), *others)
    scaled, pack = call(
        functools.partial(summed_kernel, replicas, lead),
        [shape((total, part), bf16), shape((devices, 1, 128), f32)],
        2 * total * part * width,
    )(got, hidden_padded, outputs)
    recv = lax.all_to_all(pack, ("rep", "fsdp", "exp"), split_axis=0, concat_axis=0, tiled=True)
    turned, own, *sends = call(
        functools.partial(hidden_kernel, capacity, room),
        [shape((part, total), bf16)] + [shape((slot_count, width), f32)] * fsdp,
        2 * total * part * width,
    )(scaled, weight)
    parts = [lax.ppermute(sends[d - 1], "fsdp", ring(d)) for d in range(1, fsdp)]
    weight_grad, route_grad, hidden_grad = call(
        functools.partial(final_kernel, experts, fsdp, room),
        [
            pltpu.HBM((part, width), bf16),
            pltpu.HBM((choices, tokens), f32),
            pltpu.HBM((slot_count, width), bf16),
        ],
        part * width,
        scratch=[
            VMEM((part, width), bf16),
            VMEM((choices, tokens), f32),
            VMEM((slot_count, width), bf16),
            pltpu.SemaphoreType.DMA((chunks,)),
            pltpu.SemaphoreType.DMA((2,)),
        ],
        out_specs=[any_space] * 3,
    )(recv, turned, hidden_padded, ids, taken, own, *parts)
    return route_grad.T, hidden_grad[None, None], weight_grad.reshape(1, 1, part, width)


def solution(mesh):
    placed = (
        P(("rep", "fsdp", "exp"), None),
        P(("rep", "fsdp", "exp"), None),
        P(("rep", "fsdp", "exp"), None),
        P(("rep", "fsdp"), "exp", None, None),
        P("exp", "fsdp", None),
    )

    return jax.shard_map(
        on_device,
        mesh=mesh,
        in_specs=placed,
        out_specs=(
            P(("rep", "fsdp", "exp"), None),
            P(("rep", "fsdp"), "exp", None, None),
            P("rep", "exp", "fsdp", None),
        ),
        check_vma=False,
    )
```

```python
import functools

import jax
import jax.numpy as jnp
from jax import lax
from jax.experimental import pallas as pl
from jax.experimental.pallas import tpu as pltpu
from jax.sharding import PartitionSpec as P


clip_level = 40.0
f32 = jnp.float32
bf16 = jnp.bfloat16
VMEM = pltpu.VMEM


def round_up(n, m):
    return (n + m - 1) // m * m


def iota(shape, dim):
    return lax.broadcasted_iota(jnp.int32, shape, dim)


def dot(a, b, dims):
    return lax.dot_general(a, b, (dims, ((), ())), preferred_element_type=f32)


def call(kernel, outs, flops, scratch=(), out_specs=None, in_specs=None):
    def run(*args):
        specs = in_specs or [pl.BlockSpec(memory_space=VMEM)] * len(args)
        return pl.pallas_call(
            kernel,
            out_shape=outs,
            in_specs=specs,
            out_specs=out_specs or [pl.BlockSpec(memory_space=VMEM)] * len(outs),
            scratch_shapes=list(scratch),
            compiler_params=pltpu.CompilerParams(vmem_limit_bytes=24 * 1024 * 1024),
            cost_estimate=pl.CostEstimate(flops=flops, bytes_accessed=1 << 20, transcendentals=0),
        )(*args)

    return run


def route_kernel(
    fsdp, room, lead, ids_in, probs_in, tok_in, send_ref, taken_ref, ids_ref, probs_ref, tok_ref, held, sems, out_sems
):
    loads = [
        pltpu.make_async_copy(src, dst, sems.at[i])
        for i, (src, dst) in enumerate(
            ((ids_in, ids_ref), (probs_in, probs_ref), (tok_in, tok_ref))
        )
    ]
    for load in loads:
        load.start()
    loads[0].wait()
    loads[1].wait()
    choices, tokens = ids_ref.shape
    slots = taken_ref.shape[0]
    part = tok_ref.shape[0] // fsdp
    width = send_ref.shape[2]
    slot = iota((slots, tokens), 0)
    expert = slot // room
    named = jnp.zeros((slots, tokens), jnp.bool_)
    prob = jnp.zeros((slots, tokens), f32)
    for k in range(choices):
        hit = ids_ref[k : k + 1, :] == expert
        named = named | hit
        prob = jnp.where(hit, probs_ref[k : k + 1, :].astype(f32), prob)
    earlier = (iota((tokens, tokens), 0) < iota((tokens, tokens), 1)).astype(bf16)
    order = dot(jnp.where(named, 1.0, 0.0).astype(bf16), earlier, ((1,), (0,)))
    taken = named & (order == (slot - expert * room).astype(f32))
    picker = jnp.where(taken, 1.0, 0.0)
    taken_ref[...] = picker
    prob = jnp.sum(jnp.where(taken, prob, 0.0), axis=1, keepdims=True)
    lane = iota((slots, width - part), 1)
    tail = jnp.where(lane == 0, prob, 0.0).astype(bf16)
    picker = picker.astype(bf16)
    loads[2].wait()
    stores = []
    for f in range(fsdp):
        rows = dot(picker, tok_ref[f * part : (f + 1) * part, :], ((1,), (1,))).astype(bf16)
        block = jnp.concatenate([rows, tail], axis=1)
        count = slots // room
        where = slice(f * count, (f + 1) * count)
        held[where] = block.reshape(count, room, width)
        if f == 0 and lead > 0:
            held[0] = block[lead * room : (lead + 1) * room]
            held[lead] = block[:room]
        store = pltpu.make_async_copy(held.at[where], send_ref.at[where], out_sems.at[f])
        store.start()
        stores.append(store)
    for store in stores:
        store.wait()


def spread_rows(capacity, room, hidden, rows):
    slot_count = hidden.shape[0]
    to, at = iota((rows, slot_count), 0), iota((rows, slot_count), 1)
    source, order = to // room, to % room
    spread = jnp.where((order < capacity) & (at == source * capacity + order), 1.0, 0.0).astype(bf16)
    return dot(spread, hidden, ((1,), (0,))).astype(bf16)


def outputs_kernel(capacity, room, fsdp, own_in, weight_in, *refs):
    other_refs = refs[: fsdp - 1]
    padded_ref, outputs_ref, weight_ref, own_ref, own_sem, sems = refs[fsdp - 1 :]
    part = weight_in.shape[0]
    rows = padded_ref.shape[0] // fsdp
    chunks = sems.shape[0]
    size = round_up(-(-part // chunks), 128)
    own = pltpu.make_async_copy(own_in, own_ref, own_sem)
    own.start()
    copies = []
    for c in range(chunks):
        where = slice(c * size, min((c + 1) * size, part))
        copy = pltpu.make_async_copy(weight_in.at[where, :], weight_ref.at[where, :], sems.at[c])
        copy.start()
        copies.append((where, copy))
    me = lax.axis_index("fsdp")
    own.wait()
    for d, ref in enumerate((own_ref,) + other_refs):
        group = lax.rem(me + fsdp - d, fsdp)
        to = pl.ds(pl.multiple_of(group * rows, rows), rows)
        padded_ref[to, :] = spread_rows(capacity, room, ref[...], rows)
    padded = padded_ref[...]
    for where, copy in copies:
        copy.wait()
    outputs_ref[...] = dot(padded, weight_ref[...], ((1,), (1,)))


def summed_kernel(replicas, lead, got_ref, padded_ref, outputs_ref, scaled_ref, pack_out, pack_ref, sem):
    blocks, room, width = got_ref.shape
    total = blocks * room
    part = outputs_ref.shape[1]
    got = got_ref[...].reshape(total, width)
    if lead > 0:
        near, far = got[:room], got[lead * room : (lead + 1) * room]
        got = jnp.concatenate([far, got[room : lead * room], near, got[(lead + 1) * room :]], axis=0) if lead > 1 else jnp.concatenate([far, near, got[2 * room :]], axis=0)
    rows = got[:, :part].astype(f32)
    prob = got[:, part : part + 1].astype(f32)
    scaled = (prob * rows).astype(bf16)
    scaled_ref[...] = scaled
    peak = jnp.max(jnp.abs(dot(scaled, padded_ref[...], ((0,), (0,)))))
    score = jnp.sum(rows * outputs_ref[...], axis=1, keepdims=True)
    lane = iota((total, 128), 1)
    order = iota((total, 128), 0) % room
    spread = jnp.where(lane == order, score, 0.0).reshape(blocks, room, 128)
    packed = jnp.sum(spread, axis=1)
    packed = jnp.where(iota((blocks, 128), 1) == room, peak, packed)
    for r in range(replicas):
        pack_ref[r * blocks : (r + 1) * blocks, 0, :] = packed
    store = pltpu.make_async_copy(pack_ref, pack_out, sem)
    store.start()
    store.wait()


def partial_grad(capacity, room, shift, rows, slot_count, scaled_ref, weight_ref):
    fsdp = scaled_ref.shape[0] // rows
    group = lax.rem(lax.axis_index("fsdp") + shift, fsdp)
    to, at = iota((slot_count, rows), 0), iota((slot_count, rows), 1)
    pick = jnp.where(at == to // capacity * room + to % capacity, 1.0, 0.0).astype(bf16)
    where = pl.ds(pl.multiple_of(group * rows, rows), rows)
    dense = dot(pick, scaled_ref[where, :], ((1,), (0,))).astype(bf16)
    return dot(dense, weight_ref[...], ((1,), (0,)))


def sends_kernel(capacity, room, scaled_ref, weight_ref, *send_refs):
    rows = scaled_ref.shape[0] // (len(send_refs) + 1)
    for d, ref in enumerate(send_refs):
        ref[...] = partial_grad(capacity, room, d + 1, rows, ref.shape[0], scaled_ref, weight_ref)


def keep_kernel(capacity, room, fsdp, scaled_ref, weight_ref, turned_ref, own_ref):
    rows = scaled_ref.shape[0] // fsdp
    own_ref[...] = partial_grad(capacity, room, 0, rows, own_ref.shape[0], scaled_ref, weight_ref)
    turned_ref[...] = scaled_ref[...].T


def final_kernel(experts, fsdp, room, recv_ref, turned_ref, padded_ref, ids_ref, taken_ref, own_ref, *refs):
    other_refs = refs[: fsdp - 1]
    weight_ref, route_out, hidden_out, held, route_ref, hidden_ref, sems, small_sems = refs[fsdp - 1 :]
    devices = recv_ref.shape[0]
    blocks = fsdp * experts
    replica, expert = lax.axis_index("rep"), lax.axis_index("exp")
    recv = recv_ref[...].reshape(devices, 128)
    row, lane = iota((devices, 128), 0), iota((devices, 128), 1)
    peak = jnp.max(jnp.where((lane == room) & (row % experts == expert), recv, 0.0))
    factor = jnp.minimum(1.0, clip_level / (jnp.full((1, 1), peak, f32) + 1e-06))
    chunks = sems.shape[0]
    size = turned_ref.shape[0] // chunks
    copies = []
    for c in range(chunks):
        part = slice(c * size, (c + 1) * size)
        summed = dot(turned_ref[part, :], padded_ref[...], ((1,), (0,)))
        held[part, :] = (summed * factor).astype(bf16)
        copy = pltpu.make_async_copy(held.at[part, :], weight_ref.at[part, :], sems.at[c])
        copy.start()
        copies.append(copy)
    slots, tokens = taken_ref.shape
    mine = jnp.zeros((experts, 128), f32)
    for f in range(fsdp):
        start = replica * blocks + f * experts
        mine = mine + recv_ref[pl.ds(start, experts), 0, :]
    spread = jnp.broadcast_to(mine[:, None, :], (experts, room, 128)).reshape(slots, 128)
    order = iota((slots, 128), 0) % room
    score = jnp.sum(jnp.where(iota((slots, 128), 1) == order, spread, 0.0), axis=1, keepdims=True)
    slot_expert = iota((slots, tokens), 0) // room
    found = taken_ref[...] * score
    for k in range(ids_ref.shape[0]):
        hit = ids_ref[k : k + 1, :] == slot_expert
        route_ref[k : k + 1, :] = jnp.sum(jnp.where(hit, found, 0.0), axis=0, keepdims=True)
    copies.append(pltpu.make_async_copy(route_ref, route_out, small_sems.at[0]))
    copies[-1].start()
    total = own_ref[...]
    for ref in other_refs:
        total = total + ref[...]
    hidden_ref[...] = total.astype(bf16)
    copies.append(pltpu.make_async_copy(hidden_ref, hidden_out, small_sems.at[1]))
    copies[-1].start()
    for copy in copies:
        copy.wait()


def on_device(tok_grad, expert_ids, route_probs, hidden_slots, down_weight):
    experts, fsdp, replicas = lax.axis_size("exp"), lax.axis_size("fsdp"), lax.axis_size("rep")
    slot_count, width = hidden_slots.shape[2:]
    capacity = slot_count // experts
    room = round_up(capacity, 8)
    tokens, features = tok_grad.shape
    choices = expert_ids.shape[1]
    part = down_weight.shape[1]
    padded = round_up(part + 1, 128)
    blocks, slots = fsdp * experts, experts * room
    total = blocks * room
    devices = replicas * blocks
    shape = jax.ShapeDtypeStruct
    hidden, weight = hidden_slots[0, 0], down_weight[0]
    ids = expert_ids.T
    lead = (experts - 1) // 2
    order = list(range(blocks))
    order[0], order[lead] = lead, 0

    def ring(d):
        return [(i, (i + d) % fsdp) for i in range(fsdp)]

    any_space, vmem = pl.BlockSpec(memory_space=pl.ANY), pl.BlockSpec(memory_space=VMEM)

    def stay(x):
        return pltpu.with_memory_space_constraint(x, pltpu.HBM)

    sizes = [c for c in range(8, 81, 8) if part % c == 0] or [part]
    chunks = part // sizes[-1]
    send, taken = call(
        functools.partial(route_kernel, fsdp, room, lead),
        [pltpu.HBM((blocks, room, padded), bf16), shape((slots, tokens), f32)],
        2 * slots * tokens * features,
        in_specs=[any_space] * 3,
        out_specs=[any_space, vmem],
        scratch=[
            VMEM((choices, tokens), jnp.int32),
            VMEM((choices, tokens), bf16),
            VMEM((features, tokens), bf16),
            VMEM((blocks, room, padded), bf16),
            pltpu.SemaphoreType.DMA((3,)),
            pltpu.SemaphoreType.DMA((fsdp,)),
        ],
    )(stay(ids), stay(route_probs.T), stay(tok_grad.T))
    got = lax.all_to_all(
        send,
        ("fsdp", "exp"),
        split_axis=0,
        concat_axis=0,
        axis_index_groups=[order],
        tiled=True,
    )
    others = [lax.ppermute(hidden, "fsdp", ring(d)) for d in range(1, fsdp)]
    weight_chunks = -(-part // 256)
    hidden_padded, outputs, weight = call(
        functools.partial(outputs_kernel, capacity, room, fsdp),
        [shape((total, width), bf16), shape((total, part), f32), shape((part, width), bf16)],
        2 * total * part * width,
        in_specs=[any_space] * 2 + [vmem] * (fsdp - 1),
        scratch=[
            VMEM((slot_count, width), bf16),
            pltpu.SemaphoreType.DMA,
            pltpu.SemaphoreType.DMA((weight_chunks,)),
        ],
    )(stay(hidden), stay(weight), *others)
    scaled, pack = call(
        functools.partial(summed_kernel, replicas, lead),
        [shape((total, part), bf16), pltpu.HBM((devices, 1, 128), f32)],
        2 * total * part * width,
        out_specs=[vmem, any_space],
        scratch=[VMEM((devices, 1, 128), f32), pltpu.SemaphoreType.DMA],
    )(got, hidden_padded, outputs)
    recv = lax.all_to_all(pack, ("rep", "fsdp", "exp"), split_axis=0, concat_axis=0, tiled=True)
    sends = call(
        functools.partial(sends_kernel, capacity, room),
        [shape((slot_count, width), f32)] * (fsdp - 1),
        2 * slots * part * width,
    )(scaled, weight)
    parts = [lax.ppermute(sends[d - 1], "fsdp", ring(d)) for d in range(1, fsdp)]
    turned, own = call(
        functools.partial(keep_kernel, capacity, room, fsdp),
        [shape((part, total), bf16), shape((slot_count, width), f32)],
        2 * slots * part * width,
    )(scaled, weight)
    weight_grad, route_grad, hidden_grad = call(
        functools.partial(final_kernel, experts, fsdp, room),
        [
            pltpu.HBM((part, width), bf16),
            pltpu.HBM((choices, tokens), f32),
            pltpu.HBM((slot_count, width), bf16),
        ],
        part * width,
        scratch=[
            VMEM((part, width), bf16),
            VMEM((choices, tokens), f32),
            VMEM((slot_count, width), bf16),
            pltpu.SemaphoreType.DMA((chunks,)),
            pltpu.SemaphoreType.DMA((2,)),
        ],
        out_specs=[any_space] * 3,
    )(recv, turned, hidden_padded, ids, taken, own, *parts)
    return route_grad.T, hidden_grad[None, None], weight_grad.reshape(1, 1, part, width)


def solution(mesh):
    placed = (
        P(("rep", "fsdp", "exp"), None),
        P(("rep", "fsdp", "exp"), None),
        P(("rep", "fsdp", "exp"), None),
        P(("rep", "fsdp"), "exp", None, None),
        P("exp", "fsdp", None),
    )

    return jax.shard_map(
        on_device,
        mesh=mesh,
        in_specs=placed,
        out_specs=(
            P(("rep", "fsdp", "exp"), None),
            P(("rep", "fsdp"), "exp", None, None),
            P("rep", "exp", "fsdp", None),
        ),
        check_vma=False,
    )
```
